32 devices in a mesh: shadow: 16 (over z, y, core), vocab: 2 (over x).
Axes of the slice: x: 2, y: 2, z: 4, core: 2. Of those that a mesh axis runs over, the one named last changes fastest.
Arguments:
- hidden: bfloat16 [64, 128, 2048], P('shadow'), may hold values from -18 to 18
- targets: int32 [128], replicated, may hold values from 0 to 4095
- membership: int32 [64, 4], P('shadow'), may hold values from 0 to 1, as said below
- unembedding: bfloat16 [4096, 2048], P(('shadow', 'vocab')), may hold values from -1 to 1
Outputs:
- score: float32 [64, 128], P('shadow', 'vocab')
The draws below stay inside these ranges and needn't reach their ends.
Inputs may be any that keep to these rules, and one draw needn't show every extreme that they name: `membership`: each candidate sequence is a member of exactly 32 of the shadow models.
All inputs are finite; a program needn't handle non-finite values.
Results may differ from the reference program's by a relative error of at most 0.00055.
Values may be sent and summed in bfloat16 or wider, within the bound.
A program may use at most 64 MiB of HBM per device.

```python
import math
import jax
import jax.numpy as jnp
import numpy as np
from jax import lax

D = 2048
TOK = 128
SEQ = 32
SHADOWS = 64
VOCAB = 4096
EXAMPLES = 4


def head_table(key):
    unscaled = jax.random.truncated_normal(jax.random.fold_in(key, 11), -4.0, 4.0, (VOCAB, D), jnp.float32)
    return unscaled * D ** (-0.5)


def draw_unembedding(key, part):
    return head_table(key).astype(jnp.bfloat16)


def draw_hidden(key, part):
    states = jnp.clip(jax.random.normal(jax.random.fold_in(key, 12), (SHADOWS, TOK, D), jnp.float32), -4.0, 4.0)
    return states.astype(jnp.bfloat16)


def draw_membership(key, part):
    noise = jax.random.randint(jax.random.fold_in(key, 13), (SHADOWS, EXAMPLES), 0, 1 << 20, jnp.int32)
    noise = noise * SHADOWS + jnp.arange(SHADOWS, dtype=jnp.int32)[:, None]
    ordering = jnp.argsort(noise, axis=0)
    ranking = jnp.argsort(ordering, axis=0)
    return (ranking < SHADOWS // 2).astype(jnp.int32)


def touch_ends(array, own_key, low, high):
    longest = array.shape.index(max(array.shape))
    spots = []
    for shift in (0, 1):
        where = [jax.random.randint(jax.random.fold_in(own_key, axis), (), 0, length) for axis, length in enumerate(array.shape)]
        where[longest] = (where[longest] + shift) % array.shape[longest]
        spots.append(tuple(where))
    return array.at[spots[0]].set(low).at[spots[1]].set(high)


def cumulative_ranks(number_of, lean):
    loads = [(1 << 20) // math.isqrt(standing ** lean) + 1 for standing in range(1, number_of + 1)]
    spread = 1 + sum(loads) // (1 << 30)
    return np.cumsum(np.array([max(1, weight // spread) for weight in loads]))


def skewed_ids(key, shape, amount, skew):
    grid = cumulative_ranks(amount, skew)
    ticket = jax.random.randint(jax.random.fold_in(key, 1), shape, 0, int(grid[amount - 1]))
    rank = jnp.searchsorted(jnp.asarray(grid, jnp.int32), ticket, side="right")
    return jax.random.permutation(jax.random.fold_in(key, 2), amount)[rank].astype(jnp.int32)


def setup_inputs(seed: int = 0) -> dict:
    keys = jax.random.split(jax.random.key(seed), 5)
    hidden = draw_hidden(jax.random.fold_in(keys[4], 71), 0)
    targets = touch_ends(skewed_ids(keys[1], (TOK,), VOCAB, 2), jax.random.fold_in(keys[1], 3), 0, VOCAB - 1).astype(jnp.int32)
    membership = draw_membership(jax.random.fold_in(keys[4], 71), 0)
    unembedding = draw_unembedding(jax.random.fold_in(keys[4], 71), 0)
    return dict(hidden=hidden, targets=targets, membership=membership, unembedding=unembedding)


NEG_FILL = -1e+30
VAR_FLOOR = 0.5

def reference(hidden, targets, membership, unembedding):
    columns = jnp.arange(unembedding.shape[0], dtype=jnp.int32)
    target_hit = targets.astype(jnp.int32)[:, None] == columns[None, :]

    def confidence_of(states):
        logits = lax.dot_general(states, unembedding, (((1,), (1,)), ((), ())), preferred_element_type=jnp.float32)
        target_logit = lax.optimization_barrier(jnp.sum(jnp.where(target_hit, logits, 0.0), axis=1))
        others = jnp.where(target_hit, NEG_FILL, logits)
        highest = lax.optimization_barrier(jnp.max(others, axis=1))
        summed = lax.optimization_barrier(jnp.sum(jnp.where(target_hit, 0.0, jnp.exp(others - highest[:, None])), axis=1))
        return target_logit - (highest + jnp.log(summed))
    confidence = lax.map(confidence_of, hidden)
    outside = (1 - jnp.repeat(membership, SEQ, axis=1)).astype(jnp.float32)
    weighted = outside * confidence
    first_moment = lax.optimization_barrier(jnp.sum(weighted, axis=0))
    second_moment = lax.optimization_barrier(jnp.sum(weighted * confidence, axis=0))
    out_count = SHADOWS // 2 - outside
    out_mean = (first_moment[None, :] - weighted) / out_count
    out_variance = (second_moment[None, :] - weighted * confidence) / out_count - out_mean * out_mean
    return (confidence - out_mean) * lax.rsqrt(jnp.maximum(out_variance, 0.0) + VAR_FLOOR)
```

```python
import functools

import jax
import jax.numpy as jnp
from jax import lax
from jax.experimental import pallas as pl
from jax.experimental.pallas import tpu as pltpu
from jax.sharding import PartitionSpec as P

SEQ = 32
NEG_FILL = -1e30
VAR_FLOOR = 0.5
MESH = pl.DeviceIdType.MESH

HEAD_CHUNKS = 4
HIDDEN_CHUNKS = 8


def kernel(
    nsh,
    nv,
    seq,
    hidden_hbm,
    targets_ref,
    member_ref,
    head_hbm,
    out_ref,
    hid,
    heads,
    top,
    tot,
    tgt,
    stat_send,
    stat_recv,
    mom_send,
    mom_recv,
    load_sem,
    up_send,
    down_send,
    line_recv,
    sib_send,
    sib_recv,
    hy_send,
    hy_recv,
    hx_send,
    hx_recv,
    st_send,
    st_recv,
    mo_send,
    mo_recv,
):
    nz = nsh // 4
    chunks, chunk_rows = heads.shape[1], heads.shape[3]
    head_rows = chunks * chunk_rows
    width = heads.shape[4]
    rows = hid.shape[1]
    tokens = targets_ref.shape[1]
    group = rows // tokens
    piece = rows // nv
    hparts = hy_send.shape[0]
    part = piece // hparts

    me = lax.axis_index("shadow")
    v = lax.axis_index("vocab")
    z, y, c = me // 4, (me // 2) % 2, me % 2
    sibling = me + 1 - 2 * c
    across = me + 2 - 4 * y
    has_up, has_down = z + 1 < nz, z >= 1
    one, zero = jnp.int32(1), jnp.int32(0)

    load_head = [
        pltpu.make_async_copy(
            head_hbm.at[pl.ds(j * chunk_rows, chunk_rows)], heads.at[z, j, c], load_sem.at[j]
        )
        for j in range(chunks)
    ]
    load_hidden = pltpu.make_async_copy(hidden_hbm, hid.at[0], load_sem.at[chunks])
    for copy in load_head:
        copy.start()
    load_hidden.start()

    barrier = pltpu.get_barrier_semaphore()

    def greet(s, w):
        pl.semaphore_signal(barrier, inc=1, device_id=(s, w), device_id_type=MESH)

    greet(sibling, v)
    for d in range(nv):
        if d:
            greet(me, (v + d) % nv)
        greet(across, (v + d) % nv)

    @pl.when(has_up)
    def _():
        greet(me + 4, v)

    @pl.when(has_down)
    def _():
        greet(me - 4, v)

    top[...] = jnp.full_like(top, NEG_FILL)
    tot[...] = jnp.zeros_like(tot)
    tgt[...] = jnp.zeros_like(tgt)
    pl.semaphore_wait(
        barrier, 2 * nv + jnp.where(has_up, one, zero) + jnp.where(has_down, one, zero)
    )

    def line(block, j, send, target):
        return pltpu.make_async_remote_copy(
            src_ref=heads.at[block, j, c],
            dst_ref=heads.at[block, j, c],
            send_sem=send.at[block, j],
            recv_sem=line_recv.at[block, j],
            device_id=(target, v),
            device_id_type=MESH,
        )

    def side(block, j, core):
        return pltpu.make_async_remote_copy(
            src_ref=heads.at[block, j, core],
            dst_ref=heads.at[block, j, core],
            send_sem=sib_send.at[block, j],
            recv_sem=sib_recv.at[block, j],
            device_id=(sibling, v),
            device_id_type=MESH,
        )

    def over_y(i):
        where = pl.ds(pl.multiple_of(v * piece + i * part, part), part)
        return pltpu.make_async_remote_copy(
            src_ref=hid.at[0, where],
            dst_ref=hid.at[1, where],
            send_sem=hy_send.at[i],
            recv_sem=hy_recv.at[i],
            device_id=(across, v),
            device_id_type=MESH,
        )

    def over_x(d, i, owner):
        where = pl.ds(pl.multiple_of(owner * piece + i * part, part), part)
        return pltpu.make_async_remote_copy(
            src_ref=hid.at[1, where],
            dst_ref=hid.at[1, where],
            send_sem=hx_send.at[d - 1, i],
            recv_sem=hx_recv.at[d - 1, i],
            device_id=(me, (v + d) % nv),
            device_id_type=MESH,
        )

    for j in range(chunks):
        load_head[j].wait()

        @pl.when(has_up)
        def _():
            line(z, j, up_send, me + 4).start()

        @pl.when(has_down)
        def _():
            line(z, j, down_send, me - 4).start()

        side(z, j, c).start()
    load_hidden.wait()
    for i in range(hparts):
        over_y(i).start()

    wanted = targets_ref[...]

    def fold(which, words, first, block):
        count = words.shape[0]
        logits = lax.dot_general(
            words, hid[which], (((1,), (1,)), ((), ())), preferred_element_type=jnp.float32
        )
        i = lax.broadcasted_iota(jnp.int32, (count, tokens), 0)
        core = (i // chunk_rows) % 2
        inside = first + i // (2 * chunk_rows) * chunk_rows + i % chunk_rows
        ids = (((block * 2 + y) * 2 + core) * nv + v) * head_rows + inside
        hit = ids == wanted
        for s in range(group):
            row = pl.ds(which * group + s, 1)
            mine = logits[:, s * tokens : (s + 1) * tokens]
            tgt[row] += jnp.sum(jnp.where(hit, mine, 0.0), axis=0, keepdims=True)
            others = jnp.where(hit, NEG_FILL, mine)
            before = top[row]
            raised = jnp.maximum(before, jnp.max(others, axis=0, keepdims=True))
            terms = jnp.sum(jnp.exp(others - raised), axis=0, keepdims=True)
            tot[row] = tot[row] * jnp.exp(before - raised) + terms
            top[row] = raised

    def whole_block(which, block):
        words = heads[block].reshape(2 * head_rows, width)
        fold(which, words, 0, block)

    def one_chunk(which, block, j):
        words = heads[block, j].reshape(2 * chunk_rows, width)
        fold(which, words, j * chunk_rows, block)

    for j in range(chunks):
        side(z, j, 1 - c).wait_recv()
    whole_block(0, z)

    rounds = (nz - 1) * chunks

    def turn(r, _):
        k, j = 1 + r // chunks, r % chunks
        live = r < rounds
        low, high = z - k, z + k

        @pl.when(live & (low >= 0))
        def _():
            line(low, j, up_send, me).wait_recv()

            @pl.when(has_up)
            def _():
                line(low, j, up_send, me + 4).start()

            side(low, j, c).start()

        @pl.when(live & (high < nz))
        def _():
            line(high, j, down_send, me).wait_recv()

            @pl.when(has_down)
            def _():
                line(high, j, down_send, me - 4).start()

            side(high, j, c).start()

        @pl.when(r < hparts)
        def _():
            over_y(r).wait_recv()
            for d in range(1, nv):
                over_x(d, r, v).start()

        q = r - 1
        kq, jq = 1 + (r + chunks - 1) // chunks - 1, (r + chunks - 1) % chunks

        @pl.when(r == rounds - chunks + 1)
        def _():
            for d in range(1, nv):
                for i in range(hparts):
                    over_x(d, i, (v + nv - d) % nv).wait_recv()

            def catch_up(block, _):
                away = jnp.where(block > z, block - z, z - block)

                @pl.when(away < nz - 1)
                def _():
                    whole_block(1, block)

                return 0

            lax.fori_loop(0, nz, catch_up, 0)

        def use(block):
            side(block, jq, 1 - c).wait_recv()
            one_chunk(0, block, jq)

            @pl.when(kq == nz - 1)
            def _():
                one_chunk(1, block, jq)

        @pl.when((q >= 0) & (z - kq >= 0))
        def _():
            use(z - kq)

        @pl.when((q >= 0) & (z + kq < nz))
        def _():
            use(z + kq)

        return 0

    lax.fori_loop(0, rounds + 1, turn, 0)

    for g in range(2):
        own = pl.ds(g * group, group)
        stat_send[g, 0, 0:group] = top[own]
        stat_send[g, 1, 0:group] = tot[own]
        stat_send[g, 2, 0:group] = tgt[own]

    offsets = [(dy, d) for dy in range(2) for d in range(nv) if dy or d]

    def stats(dy, d):
        return pltpu.make_async_remote_copy(
            src_ref=stat_send.at[dy],
            dst_ref=stat_recv.at[dy * nv + d],
            send_sem=st_send.at[dy * nv + d],
            recv_sem=st_recv.at[dy * nv + d],
            device_id=(across if dy else me, (v + d) % nv),
            device_id_type=MESH,
        )

    for dy, d in offsets:
        stats(dy, d).start()

    spread = jnp.zeros((group, tokens), jnp.float32)
    lane = lax.broadcasted_iota(jnp.int32, (group, tokens), 1)
    members = member_ref[...].astype(jnp.float32)
    for e in range(members.shape[1]):
        spread = jnp.where(lane // seq == e, 1.0 - members[:, e : e + 1], spread)
    outside = spread

    own = pl.ds(0, group)
    highest, summed, target_logit = top[own], tot[own], tgt[own]
    for dy, d in offsets:
        stats(dy, d).wait_recv()
        slot = dy * nv + d
        theirs = stat_recv[slot, 0, 0:group]
        raised = jnp.maximum(highest, theirs)
        summed = summed * jnp.exp(highest - raised) + stat_recv[slot, 1, 0:group] * jnp.exp(
            theirs - raised
        )
        highest = raised
        target_logit = target_logit + stat_recv[slot, 2, 0:group]
    confidence = target_logit - (highest + jnp.log(summed))
    weighted = outside * confidence

    mom_send[0:1] = jnp.sum(weighted, axis=0, keepdims=True)
    mom_send[1:2] = jnp.sum(weighted * confidence, axis=0, keepdims=True)

    def moments(d):
        return pltpu.make_async_remote_copy(
            src_ref=mom_send,
            dst_ref=mom_recv.at[d],
            send_sem=mo_send.at[d],
            recv_sem=mo_recv.at[d],
            device_id=((me + d) % nsh, v),
            device_id_type=MESH,
        )

    for d in range(1, nsh):
        moments(d).start()
    total = mom_send[0:2]
    for d in range(1, nsh):
        moments(d).wait_recv()
        total = total + mom_recv[d, 0:2]
    first_moment, second_moment = total[0:1], total[1:2]
    out_count = (group * nsh) // 2 - outside
    out_mean = (first_moment - weighted) / out_count
    out_variance = (second_moment - weighted * confidence) / out_count - out_mean * out_mean
    score = (confidence - out_mean) * lax.rsqrt(jnp.maximum(out_variance, 0.0) + VAR_FLOOR)
    keep = tokens // nv
    shifted = pltpu.roll(score, (nv - v) % nv * keep, 1)
    out_ref[...] = shifted[:, 0:keep]

    def drain(block, _):
        for j in range(chunks):
            side(block, j, c).wait_send()

            @pl.when((block <= z) & has_up)
            def _():
                line(block, j, up_send, me).wait_send()

            @pl.when((block >= z) & has_down)
            def _():
                line(block, j, down_send, me).wait_send()

        return 0

    lax.fori_loop(0, nz, drain, 0)
    for i in range(hparts):
        over_y(i).wait_send()
        for d in range(1, nv):
            over_x(d, i, v).wait_send()
    for dy, d in offsets:
        stats(dy, d).wait_send()
    for d in range(1, nsh):
        moments(d).wait_send()


def per_device(nsh, nv, hidden, targets, membership, unembedding):
    group, tokens, width = hidden.shape
    head_rows = unembedding.shape[0]
    rows = group * tokens
    nz = nsh // 4
    chunks = HEAD_CHUNKS
    hparts = max(1, min(HIDDEN_CHUNKS, rows // nv // 16))
    dma = pltpu.SemaphoreType.DMA
    hbm, vmem = pl.BlockSpec(memory_space=pl.ANY), pl.BlockSpec(memory_space=pltpu.VMEM)
    return pl.pallas_call(
        functools.partial(kernel, nsh, nv, SEQ),
        out_shape=jax.ShapeDtypeStruct((group, tokens // nv), jnp.float32),
        in_specs=[hbm, vmem, vmem, hbm],
        out_specs=vmem,
        scratch_shapes=[
            pltpu.VMEM((2, rows, width), jnp.bfloat16),
            pltpu.VMEM((nz, chunks, 2, head_rows // chunks, width), jnp.bfloat16),
            pltpu.VMEM((2 * group, tokens), jnp.float32),
            pltpu.VMEM((2 * group, tokens), jnp.float32),
            pltpu.VMEM((2 * group, tokens), jnp.float32),
            pltpu.VMEM((2, 3, 8, tokens), jnp.float32),
            pltpu.VMEM((2 * nv, 3, 8, tokens), jnp.float32),
            pltpu.VMEM((8, tokens), jnp.float32),
            pltpu.VMEM((nsh, 8, tokens), jnp.float32),
            dma((chunks + 1,)),
            dma((nz, chunks)),
            dma((nz, chunks)),
            dma((nz, chunks)),
            dma((nz, chunks)),
            dma((nz, chunks)),
            dma((hparts,)),
            dma((hparts,)),
            dma((max(1, nv - 1), hparts)),
            dma((max(1, nv - 1), hparts)),
            dma((2 * nv,)),
            dma((2 * nv,)),
            dma((nsh,)),
            dma((nsh,)),
        ],
        compiler_params=pltpu.CompilerParams(
            collective_id=0, has_side_effects=True, vmem_limit_bytes=48 * 1024 * 1024
        ),
    )(hidden.reshape(rows, width), targets.reshape(1, tokens), membership, unembedding)


def solution(mesh):
    nsh, nv = mesh.shape["shadow"], mesh.shape["vocab"]
    return jax.shard_map(
        functools.partial(per_device, nsh, nv),
        mesh=mesh,
        in_specs=(P("shadow", None, None), P(), P("shadow", None), P(("shadow", "vocab"), None)),
        out_specs=P("shadow", "vocab"),
        check_vma=False,
    )
```

```python
import functools

import jax
import jax.numpy as jnp
from jax import lax
from jax.experimental import pallas as pl
from jax.experimental.pallas import tpu as pltpu
from jax.sharding import PartitionSpec as P

SEQ = 32
NEG_FILL = -1e30
VAR_FLOOR = 0.5
MESH = pl.DeviceIdType.MESH

HEAD_CHUNKS = 8
HIDDEN_CHUNKS = 8


def kernel(
    nsh,
    nv,
    seq,
    hidden_hbm,
    targets_hbm,
    member_hbm,
    head_hbm,
    out_ref,
    targets_ref,
    member_ref,
    hid,
    heads,
    top,
    tot,
    tgt,
    acc,
    outs,
    stat_send,
    stat_recv,
    mom_send,
    mom_recv,
    load_sem,
    up_send,
    down_send,
    line_recv,
    sib_send,
    sib_recv,
    hy_send,
    hy_recv,
    hx_send,
    hx_recv,
    st_send,
    st_recv,
    mo_send,
    mo_recv,
    ou_send,
    ou_recv,
):
    nz = nsh // 4
    chunks, head_rows, slab = heads.shape[1], heads.shape[3], heads.shape[4]
    rows = hid.shape[1]
    tokens = targets_ref.shape[1]
    group = rows // tokens
    piece = rows // nv
    hparts = hy_send.shape[0]
    part = piece // hparts

    me = lax.axis_index("shadow")
    v = lax.axis_index("vocab")
    z, y, c = me // 4, (me // 2) % 2, me % 2
    sibling = me + 1 - 2 * c
    across = me + 2 - 4 * y
    has_up, has_down = z + 1 < nz, z >= 1
    one, zero = jnp.int32(1), jnp.int32(0)

    load_head = [
        pltpu.make_async_copy(
            head_hbm.at[:, pl.ds(j * slab, slab)], heads.at[z, j, c], load_sem.at[j]
        )
        for j in range(chunks)
    ]
    load_hidden = pltpu.make_async_copy(hidden_hbm, hid.at[0], load_sem.at[chunks])
    load_small = [
        pltpu.make_async_copy(targets_hbm, targets_ref, load_sem.at[chunks + 1]),
        pltpu.make_async_copy(member_hbm, member_ref, load_sem.at[chunks + 2]),
    ]
    for copy in load_head + [load_hidden] + load_small:
        copy.start()

    barrier = pltpu.get_barrier_semaphore()

    def greet(s, w):
        pl.semaphore_signal(barrier, inc=1, device_id=(s, w), device_id_type=MESH)

    greet(sibling, v)
    greet(across, v)
    for d in range(1, nv):
        greet(me, (v + d) % nv)

    @pl.when(has_up)
    def _():
        greet(me + 4, v)

    @pl.when(has_down)
    def _():
        greet(me - 4, v)

    top[...] = jnp.full_like(top, NEG_FILL)
    tot[...] = jnp.zeros_like(tot)
    tgt[...] = jnp.zeros_like(tgt)
    pl.semaphore_wait(
        barrier, nv + 1 + jnp.where(has_up, one, zero) + jnp.where(has_down, one, zero)
    )

    def line(block, j, send, target):
        return pltpu.make_async_remote_copy(
            src_ref=heads.at[block, j, c],
            dst_ref=heads.at[block, j, c],
            send_sem=send.at[block, j],
            recv_sem=line_recv.at[block, j],
            device_id=(target, v),
            device_id_type=MESH,
        )

    def side(block, j, core):
        return pltpu.make_async_remote_copy(
            src_ref=heads.at[block, j, core],
            dst_ref=heads.at[block, j, core],
            send_sem=sib_send.at[block, j],
            recv_sem=sib_recv.at[block, j],
            device_id=(sibling, v),
            device_id_type=MESH,
        )

    def over_y(i):
        where = pl.ds(pl.multiple_of(v * piece + i * part, part), part)
        return pltpu.make_async_remote_copy(
            src_ref=hid.at[0, where],
            dst_ref=hid.at[1, where],
            send_sem=hy_send.at[i],
            recv_sem=hy_recv.at[i],
            device_id=(across, v),
            device_id_type=MESH,
        )

    def over_x(d, i, owner):
        where = pl.ds(pl.multiple_of(owner * piece + i * part, part), part)
        return pltpu.make_async_remote_copy(
            src_ref=hid.at[1, where],
            dst_ref=hid.at[1, where],
            send_sem=hx_send.at[d - 1, i],
            recv_sem=hx_recv.at[d - 1, i],
            device_id=(me, (v + d) % nv),
            device_id_type=MESH,
        )

    for j in range(chunks):
        load_head[j].wait()

        @pl.when(has_up)
        def _():
            line(z, j, up_send, me + 4).start()

        @pl.when(has_down)
        def _():
            line(z, j, down_send, me - 4).start()

        side(z, j, c).start()
    load_hidden.wait()
    for i in range(hparts):
        over_y(i).start()

    for copy in load_small:
        copy.wait()
    wanted = targets_ref[...]
    lane = lax.broadcasted_iota(jnp.int32, (group, tokens), 1)
    members = member_ref[...].astype(jnp.float32)
    spread = jnp.zeros((group, tokens), jnp.float32)
    for e in range(members.shape[1]):
        spread = jnp.where(lane // seq == e, 1.0 - members[:, e : e + 1], spread)
    outs[0] = spread
    share_outs = pltpu.make_async_remote_copy(
        src_ref=outs.at[0],
        dst_ref=outs.at[1],
        send_sem=ou_send.at[0],
        recv_sem=ou_recv.at[0],
        device_id=(across, v),
        device_id_type=MESH,
    )
    share_outs.start()

    def product(which, block, j):
        words = heads[block, j].reshape(2 * head_rows, slab)
        where = pl.ds(pl.multiple_of(j * slab, slab), slab)
        return lax.dot_general(
            words,
            hid[which, :, where],
            (((1,), (1,)), ((), ())),
            preferred_element_type=jnp.float32,
        )

    def absorb(which, logits, block):
        i = lax.broadcasted_iota(jnp.int32, (2 * head_rows, tokens), 0)
        first = (block * 2 + y) * 2
        ids = ((first + i // head_rows) * nv + v) * head_rows + i % head_rows
        hit = ids == wanted
        for s in range(group):
            row = pl.ds(which * group + s, 1)
            mine = logits[:, s * tokens : (s + 1) * tokens]
            tgt[row] += jnp.sum(jnp.where(hit, mine, 0.0), axis=0, keepdims=True)
            others = jnp.where(hit, NEG_FILL, mine)
            before = top[row]
            raised = jnp.maximum(before, jnp.max(others, axis=0, keepdims=True))
            terms = jnp.sum(jnp.exp(others - raised), axis=0, keepdims=True)
            tot[row] = tot[row] * jnp.exp(before - raised) + terms
            top[row] = raised

    def whole_block(which, block):
        words = jnp.concatenate(
            [heads[block, j].reshape(2 * head_rows, slab) for j in range(chunks)], axis=1
        )
        logits = lax.dot_general(
            words, hid[which], (((1,), (1,)), ((), ())), preferred_element_type=jnp.float32
        )
        absorb(which, logits, block)

    def from_sibling(block):
        def one_wait(j, _):
            side(block, j, 1 - c).wait_recv()
            return 0

        lax.fori_loop(0, chunks, one_wait, 0)

    def fold_step(k):
        @pl.when(z - k >= 0)
        def _():
            from_sibling(z - k)
            whole_block(0, z - k)

        @pl.when((k > 0) & (z + k < nz))
        def _():
            from_sibling(z + k)
            whole_block(0, z + k)

    def arrive(k, j):
        low, high = z - k, z + k

        @pl.when(low >= 0)
        def _():
            line(low, j, up_send, me).wait_recv()

            @pl.when(has_up)
            def _():
                line(low, j, up_send, me + 4).start()

            side(low, j, c).start()

        @pl.when(high < nz)
        def _():
            line(high, j, down_send, me).wait_recv()

            @pl.when(has_down)
            def _():
                line(high, j, down_send, me - 4).start()

            side(high, j, c).start()

    last = nz - 1
    early = (last - 1) * chunks
    pace = max(1, min(2, early // hparts))

    def turn(r, _):
        arrive(1 + r // chunks, r % chunks)

        @pl.when((r % pace == pace - 1) & (r // pace < hparts))
        def _():
            i = r // pace
            over_y(i).wait_recv()
            for d in range(1, nv):
                over_x(d, i, v).start()

        @pl.when(r % chunks == 0)
        def _():
            fold_step(r // chunks)

        return 0

    lax.fori_loop(0, early, turn, 0)

    at_end = (z == 0) | (z == last)
    final = jnp.where(z == 0, jnp.int32(last), zero)
    middle = chunks // 2
    acc[...] = jnp.zeros_like(acc)

    def closing(j, _):
        arrive(last, j)

        @pl.when(j == 0)
        def _():
            fold_step(last - 1)

        @pl.when(j == middle)
        def _():
            for d in range(1, nv):
                for i in range(hparts):
                    over_x(d, i, (v + nv - d) % nv).wait_recv()

            def catch_up(block, _):
                away = jnp.where(block > z, block - z, z - block)

                @pl.when(away < last)
                def _():
                    whole_block(1, block)

                return 0

            lax.fori_loop(0, nz, catch_up, 0)

            @pl.when(at_end)
            def _():
                def missed(i, _):
                    acc[1] += product(1, final, i)
                    return 0

                lax.fori_loop(0, middle - 1, missed, 0)

        @pl.when(at_end & (j >= 1))
        def _():
            side(final, j - 1, 1 - c).wait_recv()
            acc[0] += product(0, final, j - 1)

            @pl.when(j >= middle)
            def _():
                acc[1] += product(1, final, j - 1)

        return 0

    lax.fori_loop(0, chunks, closing, 0)

    @pl.when(at_end)
    def _():
        side(final, chunks - 1, 1 - c).wait_recv()
        for which in range(2):
            absorb(which, acc[which] + product(which, final, chunks - 1), final)

    stat_send[0] = top[...]
    stat_send[1] = tot[...]
    stat_send[2] = tgt[...]

    offsets = [(dy, d) for dy in range(2) for d in range(nv) if dy or d]

    def stats(dy, d):
        return pltpu.make_async_remote_copy(
            src_ref=stat_send,
            dst_ref=stat_recv.at[dy * nv + d],
            send_sem=st_send.at[dy * nv + d],
            recv_sem=st_recv.at[dy * nv + d],
            device_id=(across if dy else me, (v + d) % nv),
            device_id_type=MESH,
        )

    for dy, d in offsets:
        stats(dy, d).start()

    share_outs.wait_recv()
    outside = jnp.concatenate([outs[0], outs[1]], axis=0)

    def seen(slot, which):
        value = stat_recv[slot, which]
        return pltpu.roll(value, group, 0) if slot >= nv else value

    highest, summed, target_logit = top[...], tot[...], tgt[...]
    for dy, d in offsets:
        stats(dy, d).wait_recv()
        slot = dy * nv + d
        theirs = seen(slot, 0)
        raised = jnp.maximum(highest, theirs)
        summed = summed * jnp.exp(highest - raised) + seen(slot, 1) * jnp.exp(theirs - raised)
        highest = raised
        target_logit = target_logit + seen(slot, 2)
    confidence = target_logit - (highest + jnp.log(summed))
    weighted = outside * confidence
    squared = weighted * confidence

    mom_send[0:1] = jnp.sum(weighted, axis=0, keepdims=True)
    mom_send[1:2] = jnp.sum(squared, axis=0, keepdims=True)

    around = [(dz, dc) for dz in range(nz) for dc in range(2) if dz or dc]

    def moments(dz, dc):
        column = (z + dz) % nz * 4 + y * 2 + (c + dc) % 2
        return pltpu.make_async_remote_copy(
            src_ref=mom_send,
            dst_ref=mom_recv.at[2 * dz + dc],
            send_sem=mo_send.at[2 * dz + dc],
            recv_sem=mo_recv.at[2 * dz + dc],
            device_id=(column, v),
            device_id_type=MESH,
        )

    for dz, dc in around:
        moments(dz, dc).start()
    total = mom_send[0:2]
    for dz, dc in around:
        moments(dz, dc).wait_recv()
        total = total + mom_recv[2 * dz + dc, 0:2]
    first_moment, second_moment = total[0:1], total[1:2]
    out_count = (group * nsh) // 2 - outside
    out_mean = (first_moment - weighted) / out_count
    out_variance = (second_moment - squared) / out_count - out_mean * out_mean
    score = (confidence - out_mean) * lax.rsqrt(jnp.maximum(out_variance, 0.0) + VAR_FLOOR)
    keep = tokens // nv
    shifted = pltpu.roll(score, (nv - v) % nv * keep, 1)
    out_ref[...] = shifted[0:group, 0:keep]

    def drain(block, _):
        for j in range(chunks):
            side(block, j, c).wait_send()

            @pl.when((block <= z) & has_up)
            def _():
                line(block, j, up_send, me).wait_send()

            @pl.when((block >= z) & has_down)
            def _():
                line(block, j, down_send, me).wait_send()

        return 0

    lax.fori_loop(0, nz, drain, 0)
    for i in range(hparts):
        over_y(i).wait_send()
        for d in range(1, nv):
            over_x(d, i, v).wait_send()
    for dy, d in offsets:
        stats(dy, d).wait_send()
    for dz, dc in around:
        moments(dz, dc).wait_send()
    share_outs.wait_send()


def per_device(nsh, nv, hidden, targets, membership, unembedding):
    group, tokens, width = hidden.shape
    head_rows = unembedding.shape[0]
    rows = group * tokens
    nz = nsh // 4
    chunks = HEAD_CHUNKS
    hparts = max(1, min(HIDDEN_CHUNKS, rows // nv // 16))
    dma = pltpu.SemaphoreType.DMA
    hbm, vmem = pl.BlockSpec(memory_space=pltpu.HBM), pl.BlockSpec(memory_space=pltpu.VMEM)
    return pl.pallas_call(
        functools.partial(kernel, nsh, nv, SEQ),
        out_shape=jax.ShapeDtypeStruct((group, tokens // nv), jnp.float32),
        in_specs=[hbm] * 4,
        out_specs=vmem,
        scratch_shapes=[
            pltpu.VMEM((1, tokens), jnp.int32),
            pltpu.VMEM(membership.shape, jnp.int32),
            pltpu.VMEM((2, rows, width), jnp.bfloat16),
            pltpu.VMEM((nz, chunks, 2, head_rows, width // chunks), jnp.bfloat16),
            pltpu.VMEM((2 * group, tokens), jnp.float32),
            pltpu.VMEM((2 * group, tokens), jnp.float32),
            pltpu.VMEM((2 * group, tokens), jnp.float32),
            pltpu.VMEM((2, 2 * head_rows, rows), jnp.float32),
            pltpu.VMEM((2, group, tokens), jnp.float32),
            pltpu.VMEM((3, 2 * group, tokens), jnp.float32),
            pltpu.VMEM((2 * nv, 3, 2 * group, tokens), jnp.float32),
            pltpu.VMEM((8, tokens), jnp.float32),
            pltpu.VMEM((2 * nz, 8, tokens), jnp.float32),
            dma((chunks + 3,)),
            dma((nz, chunks)),
            dma((nz, chunks)),
            dma((nz, chunks)),
            dma((nz, chunks)),
            dma((nz, chunks)),
            dma((hparts,)),
            dma((hparts,)),
            dma((max(1, nv - 1), hparts)),
            dma((max(1, nv - 1), hparts)),
            dma((2 * nv,)),
            dma((2 * nv,)),
            dma((2 * nz,)),
            dma((2 * nz,)),
            dma((1,)),
            dma((1,)),
        ],
        compiler_params=pltpu.CompilerParams(
            collective_id=0, has_side_effects=True, vmem_limit_bytes=67043328
        ),
    )(hidden.reshape(rows, width), targets.reshape(1, tokens), membership, unembedding)


def solution(mesh):
    nsh, nv = mesh.shape["shadow"], mesh.shape["vocab"]
    return jax.shard_map(
        functools.partial(per_device, nsh, nv),
        mesh=mesh,
        in_specs=(P("shadow", None, None), P(), P("shadow", None), P(("shadow", "vocab"), None)),
        out_specs=P("shadow", "vocab"),
        check_vma=False,
    )
```

```python
import functools

import jax
import jax.numpy as jnp
from jax import lax
from jax.experimental import pallas as pl
from jax.experimental.pallas import tpu as pltpu
from jax.sharding import PartitionSpec as P

SEQ = 32
NEG_FILL = -1e30
VAR_FLOOR = 0.5
MESH = pl.DeviceIdType.MESH

HEAD_CHUNKS = 4
HIDDEN_CHUNKS = 8


def kernel(
    nsh,
    nv,
    seq,
    hidden_hbm,
    targets_hbm,
    member_hbm,
    head_hbm,
    out_ref,
    targets_ref,
    member_ref,
    hid,
    heads,
    top,
    tot,
    tgt,
    acc,
    outs,
    stat_send,
    stat_recv,
    mom_send,
    mom_recv,
    load_sem,
    up_send,
    down_send,
    line_recv,
    sib_send,
    sib_recv,
    hy_send,
    hy_recv,
    hx_send,
    hx_recv,
    st_send,
    st_recv,
    mo_send,
    mo_recv,
    ou_send,
    ou_recv,
):
    nz = nsh // 4
    chunks, head_rows, slab = heads.shape[0], heads.shape[3], heads.shape[4]
    rows = hid.shape[1]
    tokens = targets_ref.shape[1]
    group = rows // tokens
    piece = rows // nv
    hparts = hy_send.shape[0]
    part = piece // hparts

    me = lax.axis_index("shadow")
    v = lax.axis_index("vocab")
    z, y, c = me // 4, (me // 2) % 2, me % 2
    sibling = me + 1 - 2 * c
    across = me + 2 - 4 * y
    has_up, has_down = z + 1 < nz, z >= 1
    one, zero = jnp.int32(1), jnp.int32(0)

    load_head = [
        pltpu.make_async_copy(
            head_hbm.at[:, pl.ds(j * slab, slab)], heads.at[j, z, c], load_sem.at[j]
        )
        for j in range(chunks)
    ]
    load_hidden = pltpu.make_async_copy(hidden_hbm, hid.at[0], load_sem.at[chunks])
    load_small = [
        pltpu.make_async_copy(targets_hbm, targets_ref, load_sem.at[chunks + 1]),
        pltpu.make_async_copy(member_hbm, member_ref, load_sem.at[chunks + 2]),
    ]
    for copy in load_head + [load_hidden] + load_small:
        copy.start()

    barrier = pltpu.get_barrier_semaphore()

    def greet(s, w):
        pl.semaphore_signal(barrier, inc=1, device_id=(s, w), device_id_type=MESH)

    greet(sibling, v)
    greet(across, v)
    for d in range(1, nv):
        greet(me, (v + d) % nv)

    @pl.when(has_up)
    def _():
        greet(me + 4, v)

    @pl.when(has_down)
    def _():
        greet(me - 4, v)

    top[...] = jnp.full_like(top, NEG_FILL)
    tot[...] = jnp.zeros_like(tot)
    tgt[...] = jnp.zeros_like(tgt)
    pl.semaphore_wait(
        barrier, nv + 1 + jnp.where(has_up, one, zero) + jnp.where(has_down, one, zero)
    )

    def line(block, j, send, target):
        return pltpu.make_async_remote_copy(
            src_ref=heads.at[j, block, c],
            dst_ref=heads.at[j, block, c],
            send_sem=send.at[block, j],
            recv_sem=line_recv.at[block, j],
            device_id=(target, v),
            device_id_type=MESH,
        )

    def side(block, j, core):
        return pltpu.make_async_remote_copy(
            src_ref=heads.at[j, block, core],
            dst_ref=heads.at[j, block, core],
            send_sem=sib_send.at[block, j],
            recv_sem=sib_recv.at[block, j],
            device_id=(sibling, v),
            device_id_type=MESH,
        )

    def over_y(i):
        where = pl.ds(pl.multiple_of(v * piece + i * part, part), part)
        return pltpu.make_async_remote_copy(
            src_ref=hid.at[0, where],
            dst_ref=hid.at[1, where],
            send_sem=hy_send.at[i],
            recv_sem=hy_recv.at[i],
            device_id=(across, v),
            device_id_type=MESH,
        )

    def over_x(d, i, owner):
        where = pl.ds(pl.multiple_of(owner * piece + i * part, part), part)
        return pltpu.make_async_remote_copy(
            src_ref=hid.at[1, where],
            dst_ref=hid.at[1, where],
            send_sem=hx_send.at[d - 1, i],
            recv_sem=hx_recv.at[d - 1, i],
            device_id=(me, (v + d) % nv),
            device_id_type=MESH,
        )

    for j in range(chunks):
        load_head[j].wait()

        @pl.when(has_up)
        def _():
            line(z, j, up_send, me + 4).start()

        @pl.when(has_down)
        def _():
            line(z, j, down_send, me - 4).start()

        side(z, j, c).start()
    load_hidden.wait()
    for i in range(hparts):
        over_y(i).start()

    for copy in load_small:
        copy.wait()
    wanted = targets_ref[...]
    lane = lax.broadcasted_iota(jnp.int32, (group, tokens), 1)
    members = member_ref[...].astype(jnp.float32)
    spread = jnp.zeros((group, tokens), jnp.float32)
    for e in range(members.shape[1]):
        spread = jnp.where(lane // seq == e, 1.0 - members[:, e : e + 1], spread)
    outs[0] = spread
    share_outs = pltpu.make_async_remote_copy(
        src_ref=outs.at[0],
        dst_ref=outs.at[1],
        send_sem=ou_send.at[0],
        recv_sem=ou_recv.at[0],
        device_id=(across, v),
        device_id_type=MESH,
    )
    share_outs.start()

    def product(which, block, j):
        words = heads[j, block].reshape(2 * head_rows, slab)
        where = pl.ds(pl.multiple_of(j * slab, slab), slab)
        return lax.dot_general(
            words,
            hid[which, :, where],
            (((1,), (1,)), ((), ())),
            preferred_element_type=jnp.float32,
        )

    def absorb(row0, logits, block):
        count = logits.shape[0]
        i = lax.broadcasted_iota(jnp.int32, (count, tokens), 0)
        first = (block + i // (2 * head_rows)) * 4 + y * 2 + i // head_rows % 2
        ids = (first * nv + v) * head_rows + i % head_rows
        hit = ids == wanted
        for s in range(logits.shape[1] // tokens):
            row = pl.ds(row0 + s, 1)
            mine = logits[:, s * tokens : (s + 1) * tokens]
            tgt[row] += jnp.sum(jnp.where(hit, mine, 0.0), axis=0, keepdims=True)
            others = jnp.where(hit, NEG_FILL, mine)
            before = top[row]
            raised = jnp.maximum(before, jnp.max(others, axis=0, keepdims=True))
            terms = jnp.sum(jnp.exp(others - raised), axis=0, keepdims=True)
            tot[row] = tot[row] * jnp.exp(before - raised) + terms
            top[row] = raised

    def fold_blocks(block, count, which, start, size):
        words = jnp.concatenate(
            [
                heads[j, pl.ds(block, count)].reshape(count * 2 * head_rows, slab)
                for j in range(chunks)
            ],
            axis=1,
        )
        logits = lax.dot_general(
            words,
            hid[which, pl.ds(start, size)],
            (((1,), (1,)), ((), ())),
            preferred_element_type=jnp.float32,
        )
        absorb(which * group + start // tokens, logits, block)

    def whole_block(which, block):
        fold_blocks(block, 1, which, 0, rows)

    def from_sibling(block):
        def one_wait(j, _):
            side(block, j, 1 - c).wait_recv()
            return 0

        lax.fori_loop(0, chunks, one_wait, 0)

    def fold_step(k):
        @pl.when(z - k >= 0)
        def _():
            from_sibling(z - k)
            whole_block(0, z - k)

        @pl.when((k > 0) & (z + k < nz))
        def _():
            from_sibling(z + k)
            whole_block(0, z + k)

    def arrive(k, j):
        low, high = z - k, z + k

        @pl.when(low >= 0)
        def _():
            line(low, j, up_send, me).wait_recv()

            @pl.when(has_up)
            def _():
                line(low, j, up_send, me + 4).start()

            side(low, j, c).start()

        @pl.when(high < nz)
        def _():
            line(high, j, down_send, me).wait_recv()

            @pl.when(has_down)
            def _():
                line(high, j, down_send, me - 4).start()

            side(high, j, c).start()

    last = nz - 1
    early = (last - 1) * chunks
    pace = max(1, min(2, early // hparts))

    def turn(r, _):
        arrive(1 + r // chunks, r % chunks)

        @pl.when((r % pace == pace - 1) & (r // pace < hparts))
        def _():
            i = r // pace
            over_y(i).wait_recv()
            for d in range(1, nv):
                over_x(d, i, v).start()

        @pl.when(r % chunks == 0)
        def _():
            fold_step(r // chunks)

        return 0

    lax.fori_loop(0, early, turn, 0)

    at_end = (z == 0) | (z == last)
    final = jnp.where(z == 0, jnp.int32(last), zero)
    middle = chunks // 2
    by_piece = piece % tokens == 0
    unit = piece if by_piece else rows
    base = jnp.where(z == last, one, zero)
    acc[...] = jnp.zeros_like(acc)

    def closing(j, _):
        arrive(last, j)

        @pl.when(j == 0)
        def _():
            fold_step(last - 1)

        def catch_up(owner):
            start = pl.multiple_of(owner * unit, unit)
            fold_blocks(base, last, 1, start, unit)

            @pl.when(jnp.logical_not(at_end))
            def _():
                fold_blocks(last, 1, 1, start, unit)

        if by_piece:

            @pl.when(j == 0)
            def _():
                catch_up(v)

        @pl.when(j == middle)
        def _():
            for d in range(1, nv):
                for i in range(hparts):
                    over_x(d, i, (v + nv - d) % nv).wait_recv()
                if by_piece:
                    catch_up((v + nv - d) % nv)
            if not by_piece:
                catch_up(zero)

            @pl.when(at_end)
            def _():
                def missed(i, _):
                    acc[1] += product(1, final, i)
                    return 0

                lax.fori_loop(0, middle - 1, missed, 0)

        @pl.when(at_end & (j >= 1))
        def _():
            side(final, j - 1, 1 - c).wait_recv()
            acc[0] += product(0, final, j - 1)

            @pl.when(j >= middle)
            def _():
                acc[1] += product(1, final, j - 1)

        return 0

    lax.fori_loop(0, chunks, closing, 0)

    @pl.when(at_end)
    def _():
        side(final, chunks - 1, 1 - c).wait_recv()
        for which in range(2):
            absorb(which * group, acc[which] + product(which, final, chunks - 1), final)

    stat_send[0] = top[...]
    stat_send[1] = tot[...]
    stat_send[2] = tgt[...]

    offsets = [(dy, d) for dy in range(2) for d in range(nv) if dy or d]

    def stats(dy, d):
        return pltpu.make_async_remote_copy(
            src_ref=stat_send,
            dst_ref=stat_recv.at[dy * nv + d],
            send_sem=st_send.at[dy * nv + d],
            recv_sem=st_recv.at[dy * nv + d],
            device_id=(across if dy else me, (v + d) % nv),
            device_id_type=MESH,
        )

    for dy, d in offsets:
        stats(dy, d).start()

    share_outs.wait_recv()
    outside = jnp.concatenate([outs[0], outs[1]], axis=0)

    def seen(slot, which):
        value = stat_recv[slot, which]
        return pltpu.roll(value, group, 0) if slot >= nv else value

    highest, summed, target_logit = top[...], tot[...], tgt[...]
    for dy, d in offsets:
        stats(dy, d).wait_recv()
        slot = dy * nv + d
        theirs = seen(slot, 0)
        raised = jnp.maximum(highest, theirs)
        summed = summed * jnp.exp(highest - raised) + seen(slot, 1) * jnp.exp(theirs - raised)
        highest = raised
        target_logit = target_logit + seen(slot, 2)
    confidence = target_logit - (highest + jnp.log(summed))
    weighted = outside * confidence
    squared = weighted * confidence

    mom_send[0:1] = jnp.sum(weighted, axis=0, keepdims=True)
    mom_send[1:2] = jnp.sum(squared, axis=0, keepdims=True)

    around = [(dz, dc) for dz in range(nz) for dc in range(2) if dz or dc]

    def moments(dz, dc):
        column = (z + dz) % nz * 4 + y * 2 + (c + dc) % 2
        return pltpu.make_async_remote_copy(
            src_ref=mom_send,
            dst_ref=mom_recv.at[2 * dz + dc],
            send_sem=mo_send.at[2 * dz + dc],
            recv_sem=mo_recv.at[2 * dz + dc],
            device_id=(column, v),
            device_id_type=MESH,
        )

    for dz, dc in around:
        moments(dz, dc).start()
    total = mom_send[0:2]
    for dz, dc in around:
        moments(dz, dc).wait_recv()
        total = total + mom_recv[2 * dz + dc, 0:2]
    first_moment, second_moment = total[0:1], total[1:2]
    out_count = (group * nsh) // 2 - outside
    out_mean = (first_moment - weighted) / out_count
    out_variance = (second_moment - squared) / out_count - out_mean * out_mean
    score = (confidence - out_mean) * lax.rsqrt(jnp.maximum(out_variance, 0.0) + VAR_FLOOR)
    keep = tokens // nv
    shifted = pltpu.roll(score, (nv - v) % nv * keep, 1)
    out_ref[...] = shifted[0:group, 0:keep]

    def drain(block, _):
        for j in range(chunks):
            side(block, j, c).wait_send()

            @pl.when((block <= z) & has_up)
            def _():
                line(block, j, up_send, me).wait_send()

            @pl.when((block >= z) & has_down)
            def _():
                line(block, j, down_send, me).wait_send()

        return 0

    lax.fori_loop(0, nz, drain, 0)
    for i in range(hparts):
        over_y(i).wait_send()
        for d in range(1, nv):
            over_x(d, i, v).wait_send()
    for dy, d in offsets:
        stats(dy, d).wait_send()
    for dz, dc in around:
        moments(dz, dc).wait_send()
    share_outs.wait_send()


def per_device(nsh, nv, hidden, targets, membership, unembedding):
    group, tokens, width = hidden.shape
    head_rows = unembedding.shape[0]
    rows = group * tokens
    nz = nsh // 4
    chunks = HEAD_CHUNKS
    hparts = max(1, min(HIDDEN_CHUNKS, rows // nv // 16))
    dma = pltpu.SemaphoreType.DMA
    hbm, vmem = pl.BlockSpec(memory_space=pltpu.HBM), pl.BlockSpec(memory_space=pltpu.VMEM)
    return pl.pallas_call(
        functools.partial(kernel, nsh, nv, SEQ),
        out_shape=jax.ShapeDtypeStruct((group, tokens // nv), jnp.float32),
        in_specs=[hbm] * 4,
        out_specs=vmem,
        scratch_shapes=[
            pltpu.VMEM((1, tokens), jnp.int32),
            pltpu.VMEM(membership.shape, jnp.int32),
            pltpu.VMEM((2, rows, width), jnp.bfloat16),
            pltpu.VMEM((chunks, nz, 2, head_rows, width // chunks), jnp.bfloat16),
            pltpu.VMEM((2 * group, tokens), jnp.float32),
            pltpu.VMEM((2 * group, tokens), jnp.float32),
            pltpu.VMEM((2 * group, tokens), jnp.float32),
            pltpu.VMEM((2, 2 * head_rows, rows), jnp.float32),
            pltpu.VMEM((2, group, tokens), jnp.float32),
            pltpu.VMEM((3, 2 * group, tokens), jnp.float32),
            pltpu.VMEM((2 * nv, 3, 2 * group, tokens), jnp.float32),
            pltpu.VMEM((8, tokens), jnp.float32),
            pltpu.VMEM((2 * nz, 8, tokens), jnp.float32),
            dma((chunks + 3,)),
            dma((nz, chunks)),
            dma((nz, chunks)),
            dma((nz, chunks)),
            dma((nz, chunks)),
            dma((nz, chunks)),
            dma((hparts,)),
            dma((hparts,)),
            dma((max(1, nv - 1), hparts)),
            dma((max(1, nv - 1), hparts)),
            dma((2 * nv,)),
            dma((2 * nv,)),
            dma((2 * nz,)),
            dma((2 * nz,)),
            dma((1,)),
            dma((1,)),
        ],
        compiler_params=pltpu.CompilerParams(
            collective_id=0, has_side_effects=True, vmem_limit_bytes=67043328
        ),
    )(hidden.reshape(rows, width), targets.reshape(1, tokens), membership, unembedding)


def solution(mesh):
    nsh, nv = mesh.shape["shadow"], mesh.shape["vocab"]
    return jax.shard_map(
        functools.partial(per_device, nsh, nv),
        mesh=mesh,
        in_specs=(P("shadow", None, None), P(), P("shadow", None), P(("shadow", "vocab"), None)),
        out_specs=P("shadow", "vocab"),
        check_vma=False,
    )
```
